256 devices in a mesh: cosmo: 2 (over y), shell: 4 (over x), band: 32 (over z, core).
Axes of the slice: x: 4, y: 2, z: 16, core: 2. Of those that a mesh axis runs over, the one named last changes fastest.
The devices are a block of a 4x16x16 slice.
Arguments:
- cycle_modes: float32 [1024, 128, 2, 128], P(('cosmo', 'shell'), 'band'), parts along dimension 0, may hold values from -6 to 6
- cycle_weight: float32 [128], P('band'), may hold values from 0.5 to 2
- legendre: float32 [128, 128, 4096], P('band'), may hold values from -0.5 to 0.5
- spin_plus: bfloat16 [128, 128, 4096], P('band'), may hold values from -0.5 to 0.5
- spin_minus: bfloat16 [128, 128, 4096], P('band'), may hold values from -0.5 to 0.5
- window: float32 [512, 4096], P('shell'), may hold values from 0.3 to 3
- lensing: float32 [1024], P(('cosmo', 'shell')), parts along dimension 0, may hold values from 0.05 to 0.5
- source_shell: int32 [8], P('cosmo'), parts along dimension 0, may hold values from 384 to 511
Outputs:
- lensing_maps: float32 [8, 3, 128, 2, 128], P(('cosmo', 'shell'), None, 'band'), parts along dimension 0
The draws below stay inside these ranges and needn't reach their ends.
There are 2 independent parts, one for each index of `cosmo`. The reference program is written for one: setup_inputs(seed, part) draws one part's arguments, and reference() takes and returns one part's arrays. A program takes and returns all parts, laid end to end along the dimension named above; an argument that names none is the same for every part. Nothing has to cross between parts.
All inputs are finite; a program needn't handle non-finite values.
Results may differ from the reference program's by a relative error of at most 0.00073.
Values sent between devices are 32-bit elements; how exact they have to be, the bound alone decides.
A program may use at most 64 MiB of HBM per device.

```python
import math
import jax
import jax.numpy as jnp
from jax import lax

L = 4096
BINS = 4
SH_DEV = 128
SHELLS = 512
CYCLES = 128
ORDERS = 128
N_SHELL = 4


def with_ends(array, stream_key, smallest, largest):
    dims = array.shape
    index_at = [jax.random.randint(jax.random.fold_in(stream_key, axis), (), 0, dims[axis]) for axis in range(len(dims))]
    array = array.at[tuple(index_at)].set(smallest)
    longest = dims.index(max(dims))
    index_at[longest] = (index_at[longest] + 1) % dims[longest]
    return array.at[tuple(index_at)].set(largest)


def steps_of(key, extent, split, least, largest):
    factor_of = 1.0
    for axis_at, parts in split:
        draws = jax.random.uniform(jax.random.fold_in(jax.random.fold_in(key, 6), axis_at), (parts,), jnp.float32, least / len(split), largest / len(split))
        factor_of = factor_of * jnp.repeat(jnp.exp(draws), extent[axis_at] // parts).reshape((-1,) + (1,) * (len(extent) - 1 - axis_at))
    return factor_of


def gaussian(key, shape, spread, bound, split=(), kind=jnp.bfloat16):
    result = spread * jax.random.normal(key, shape, jnp.float32)
    if split:
        result = result * steps_of(key, shape, split, -0.22, 0.18)
    return jnp.clip(result, -bound, bound).astype(kind)


def setup_inputs(seed: int = 0, part: int = 0) -> dict:
    arg_keys = jax.random.split(jax.random.key(seed), 9)
    part_keys = jax.random.split(jax.random.fold_in(arg_keys[8], part), 9)
    cycle_modes = gaussian(part_keys[0], (SHELLS, CYCLES, 2, ORDERS), 1.0, 6.0, ((0, 4), (1, 32)), jnp.float32)
    cycle_weight = jnp.clip(jnp.exp(math.log(2.0) - 1.3862944 * jax.random.uniform(arg_keys[1], (CYCLES,), jnp.float32) ** steps_of(arg_keys[1], (CYCLES,), ((0, 32),), -0.2, 0.2)), 0.5, 2.0)
    legendre = gaussian(arg_keys[2], (ORDERS, CYCLES, L), CYCLES ** -0.5, 0.5, ((0, 32),), jnp.float32)
    spin_plus = gaussian(arg_keys[3], (ORDERS, CYCLES, L), CYCLES ** -0.5, 0.5, ((0, 32),))
    spin_minus = gaussian(arg_keys[4], (ORDERS, CYCLES, L), CYCLES ** -0.5, 0.5, ((0, 32),))
    window = jnp.clip(jnp.exp(math.log(3.0) - 2.3025851 * jax.random.uniform(arg_keys[5], (SHELLS, L), jnp.float32) ** steps_of(arg_keys[5], (SHELLS, L), ((0, 4),), -0.2, 0.2)), 0.3, 3.0)
    lensing = jnp.clip(jnp.exp(math.log(0.5) - 2.3025851 * jax.random.uniform(part_keys[6], (SHELLS,), jnp.float32) ** steps_of(part_keys[6], (SHELLS,), ((0, 4),), -0.2, 0.2)), 0.05, 0.5)
    source_shell = with_ends(jax.random.randint(part_keys[7], (BINS,), 3 * SHELLS // 4, SHELLS), jax.random.fold_in(part_keys[7], 1), 3 * SHELLS // 4, SHELLS - 1).astype(jnp.int32)
    return dict(cycle_modes=cycle_modes, cycle_weight=cycle_weight, legendre=legendre, spin_plus=spin_plus, spin_minus=spin_minus, window=window, lensing=lensing, source_shell=source_shell)


def reference(cycle_modes, cycle_weight, legendre, spin_plus, spin_minus, window, lensing, source_shell):
    highest = lax.Precision.HIGHEST
    weighted = cycle_modes * cycle_weight[None, :, None, None]
    degree = jnp.arange(L).astype(jnp.float32)
    shell_ids = jnp.arange(SHELLS).astype(jnp.int32)
    source = source_shell.astype(jnp.int32)
    efficiency = lensing[None, :] * jnp.maximum(source[:, None] - shell_ids[None, :], 0).astype(jnp.float32) / (source[:, None] + 1).astype(jnp.float32)
    shear_ratio = jnp.where(degree >= 2.0, jnp.sqrt((degree + 2.0) * (degree - 1.0) / jnp.maximum(degree * (degree + 1.0), 1.0)), 0.0)
    plus_table = spin_plus.astype(jnp.float32)
    minus_table = spin_minus.astype(jnp.float32)
    summed = jnp.zeros((BINS, 3, CYCLES, 2, ORDERS), jnp.float32)
    for group in range(N_SHELL):
        first = group * SH_DEV
        harmonic = jnp.einsum('srcm,mrl->smcl', weighted[first:first + SH_DEV], legendre, precision=highest)
        factor = window[first:first + SH_DEV][:, None, None, :]
        binned = jnp.einsum('bs,smcl->bmcl', efficiency[:, first:first + SH_DEV], harmonic * factor, precision=highest)
        shear_coef = (-shear_ratio[None, None, None, :] * binned).astype(jnp.bfloat16).astype(jnp.float32)
        kappa_map = jnp.einsum('bmcl,mrl->brcm', binned, legendre, precision=highest)
        plus_map = jnp.einsum('bmcl,mrl->brcm', shear_coef, plus_table, precision=highest)
        minus_map = jnp.einsum('bmcl,mrl->brcm', shear_coef, minus_table, precision=highest)
        rotated = jnp.stack([-minus_map[:, :, 1], minus_map[:, :, 0]], axis=2)
        summed = summed + jnp.stack([kappa_map, plus_map, rotated], axis=1)
    return summed
```

```python
import functools

import jax
import jax.numpy as jnp
from jax import lax
from jax.experimental import pallas as pl
from jax.experimental.pallas import tpu as pltpu
from jax.sharding import PartitionSpec as P

MESH = pl.DeviceIdType.MESH
LANES = 128
TILE = 256


def roll(x, shift, axis):
    return pltpu.roll(x, shift, axis)


def kernel(
    n_band,
    n_shell,
    modes,
    weight,
    legendre,
    plus,
    minus,
    window,
    lensing,
    source,
    out,
    modes_v,
    send_v,
    recv_v,
    leg_v,
    tab_v,
    win_v,
    eff_v,
    fac_v,
    a_v,
    x_v,
    h0_v,
    h1_v,
    w_v,
    p1s_v,
    p1r_v,
    p2t_v,
    p2s_v,
    p2r_v,
    in_sem,
    leg_sem,
    plus_sem,
    minus_sem,
    send_sem,
    recv_sem,
    p1s_sem,
    p1r_sem,
    p2s_sem,
    p2r_sem,
):
    f32, bf16 = jnp.float32, jnp.bfloat16
    band, shell = lax.axis_index("band"), lax.axis_index("shell")
    chips = n_band // 2
    chip, core = band // 2, band % 2
    own = legendre.shape[0]
    cycles = legendre.shape[1]
    degrees = legendre.shape[2]
    shells = window.shape[0]
    bins = n_shell
    rows = 2 * (cycles // n_band)

    def peer(j):
        k = j // 2
        step = ((k + 1) // 2) * (2 * (k % 2) - 1)
        return 2 * ((chip + step + chips) % chips) + (core + j) % 2

    get_modes = pltpu.make_async_copy(modes, modes_v, in_sem.at[0])
    get_window = pltpu.make_async_copy(window, win_v, in_sem.at[1])
    get_modes.start()

    barrier = pltpu.get_barrier_semaphore()

    @pl.loop(1, n_band)
    def _(j):
        pl.semaphore_signal(barrier, inc=1, device_id={"band": peer(j)}, device_id_type=MESH)

    for dx in range(1, n_shell):
        pl.semaphore_signal(
            barrier, inc=1, device_id={"shell": (shell + dx) % n_shell}, device_id_type=MESH
        )

    def get_legendre(i):
        return pltpu.make_async_copy(legendre.at[i], leg_v.at[i], leg_sem.at[i])

    def get_plus(i):
        at = pl.ds(2 * cycles, cycles)
        return pltpu.make_async_copy(plus.at[i], tab_v.at[i, at], plus_sem.at[i])

    def get_minus(i):
        at = pl.ds(3 * cycles, cycles)
        return pltpu.make_async_copy(minus.at[i], tab_v.at[i, at], minus_sem.at[i])

    for i in range(own):
        get_legendre(i).start()
    get_window.start()
    for i in range(own):
        get_plus(i).start()
        get_minus(i).start()

    get_modes.wait()
    for k in range(rows):
        block = modes_v[pl.ds(k, shells, stride=rows), :] * weight[k // 2]
        send_v[pl.ds(k, LANES, stride=rows), :] = block.T

    pl.semaphore_wait(barrier, n_band - 1 + n_shell - 1)

    def order_copy(i, d):
        return pltpu.make_async_remote_copy(
            src_ref=send_v.at[pl.ds(pl.multiple_of((own * d + i) * rows, rows), rows)],
            dst_ref=recv_v.at[pl.ds(pl.multiple_of((i * n_band + band) * rows, rows), rows)],
            send_sem=send_sem.at[i],
            recv_sem=recv_sem.at[i],
            device_id={"band": d},
            device_id_type=MESH,
        )

    @pl.loop(0, own)
    def _(i):
        @pl.loop(1, n_band)
        def _(j):
            order_copy(i, peer(j)).start()

        recv_v[pl.ds(pl.multiple_of((i * n_band + band) * rows, rows), rows), :] = send_v[
            pl.ds(pl.multiple_of((own * band + i) * rows, rows), rows), :
        ]

    def all_orders(i):
        n = (n_band - 1) * rows
        at = pl.ds(pl.multiple_of(i * n_band * rows, rows), n)
        return pltpu.make_async_remote_copy(
            src_ref=recv_v.at[at],
            dst_ref=recv_v.at[at],
            send_sem=send_sem.at[i],
            recv_sem=recv_sem.at[i],
            device_id={"band": peer(1)},
            device_id_type=MESH,
        )

    spread = jnp.broadcast_to(lensing[0:1, :], (LANES, LANES)).T
    shell_id = shell * shells + lax.broadcasted_iota(jnp.int32, (shells, LANES), 0)
    for b in range(bins):
        at = jnp.full((shells, LANES), source[b], jnp.int32)
        eff_v[b] = spread * jnp.maximum(at - shell_id, 0).astype(f32) / (at + 1).astype(f32)

    sub = lax.broadcasted_iota(jnp.int32, (8, LANES), 0)
    even = sub % 2 == 0

    @pl.loop(0, degrees // LANES)
    def _(k):
        at = pl.multiple_of(k * LANES, LANES)
        degree = (at + lax.broadcasted_iota(jnp.int32, (8, LANES), 1)).astype(f32)
        ratio = jnp.where(
            degree >= 2.0,
            jnp.sqrt((degree + 2.0) * (degree - 1.0) / jnp.maximum(degree * (degree + 1.0), 1.0)),
            0.0,
        )
        turned = jnp.where(even, ratio, -ratio)
        fac_v[:, pl.ds(at, LANES)] = jnp.where(
            sub < 2, 1.0, jnp.where(sub < 4, -ratio, turned)
        )

    @pl.loop(0, own)
    def _(i):
        get_legendre(i).wait()

        @pl.loop(0, cycles // 16)
        def _(k):
            at = pl.ds(pl.multiple_of(k * 16, 16), 16)
            value = leg_v[i, at, :]
            high = value.astype(bf16)
            tab_v[i, at, :] = high
            at = pl.ds(pl.multiple_of(cycles + k * 16, 16), 16)
            tab_v[i, at, :] = (value - high.astype(f32)).astype(bf16)

    get_window.wait()

    def transform(i, t, h_v):
        table = tab_v[i, 0 : 2 * cycles, pl.ds(pl.multiple_of(t * TILE, TILE), TILE)]
        h_v[...] = jnp.dot(a_v[...], table, preferred_element_type=f32) + jnp.dot(
            x_v[...], table[:cycles], preferred_element_type=f32
        )

    def bin_sums(t, h_v):
        for k in range(TILE // LANES):
            lanes = pl.ds(pl.multiple_of(t * TILE + k * LANES, LANES), LANES)
            sums = [[None, None] for _ in range(bins)]
            for g in range(shells // 8):
                at = slice(8 * g, 8 * g + 8)
                w = win_v[at, lanes]
                for c in range(2):
                    h = h_v[c * shells + 8 * g : c * shells + 8 * g + 8, k * LANES : (k + 1) * LANES]
                    hw = h * w
                    for b in range(bins):
                        term = hw * eff_v[b, at, :]
                        sums[b][c] = term if g == 0 else sums[b][c] + term
            fac = fac_v[:, lanes]
            parts = []
            for b in range(bins):
                x, y = sums[b]
                z = jnp.where(even, x + roll(x, 1, 0), y + roll(y, 1, 0))
                z = z + roll(z, 2, 0)
                z = z + roll(z, 4, 0)
                turned = roll(z, 1, 0)
                v = jnp.where((sub == 4) | (sub == 5), turned, z) * fac
                low = z - z.astype(bf16).astype(f32)
                parts.append(jnp.where(sub >= 6, low, v))
            w_v[:, lanes] = jnp.concatenate(parts, axis=0).astype(bf16)

    tiles = degrees // TILE
    chunk = 1024

    @pl.loop(0, own)
    def _(i):
        all_orders(i).wait_recv()
        for c in range(2):
            x = recv_v[pl.ds(i * n_band * rows + c, cycles, stride=2), :].T
            high = x.astype(bf16)
            at = slice(c * shells, (c + 1) * shells)
            a_v[at, :cycles] = high
            a_v[at, cycles:] = high
            x_v[at, :] = (x - high.astype(f32)).astype(bf16)

        transform(i, 0, h0_v)

        @pl.loop(0, tiles // 2 - 1)
        def _(t):
            transform(i, 2 * t + 1, h1_v)
            bin_sums(2 * t, h0_v)
            transform(i, 2 * t + 2, h0_v)
            bin_sums(2 * t + 1, h1_v)

        transform(i, tiles - 1, h1_v)
        bin_sums(tiles - 2, h0_v)
        bin_sums(tiles - 1, h1_v)

        get_plus(i).wait()
        get_minus(i).wait()
        maps = None
        for k in range(degrees // chunk):
            at = slice(k * chunk, (k + 1) * chunk)
            term = lax.dot_general(
                tab_v[i, :, at],
                w_v[:, at],
                (((1,), (1,)), ((), ())),
                preferred_element_type=f32,
            )
            maps = term if maps is None else maps + term
        maps = maps.T
        for b in range(bins):
            kh, kl, p, m = (
                maps[8 * b : 8 * b + 8, q * cycles : (q + 1) * cycles] for q in range(4)
            )
            p1s_v[i, b] = jnp.where(
                sub < 2, kh + kl + roll(kh, 2, 0), jnp.where(sub < 4, p, m)
            )
        for dx in range(1, n_shell):
            d = (shell + dx) % n_shell
            pltpu.make_async_remote_copy(
                src_ref=p1s_v.at[i, d],
                dst_ref=p1r_v.at[i, shell],
                send_sem=p1s_sem.at[i],
                recv_sem=p1r_sem.at[i],
                device_id={"shell": d},
                device_id_type=MESH,
            ).start()
        p1r_v[i, shell] = p1s_v[i, shell]

    def all_bins(i):
        return pltpu.make_async_remote_copy(
            src_ref=p1r_v.at[i, pl.ds(0, n_shell - 1)],
            dst_ref=p1r_v.at[i, pl.ds(0, n_shell - 1)],
            send_sem=p1s_sem.at[i],
            recv_sem=p1r_sem.at[i],
            device_id={"shell": (shell + 1) % n_shell},
            device_id_type=MESH,
        )

    summed = []
    for i in range(own):
        all_bins(i).wait_recv()
        total = p1r_v[i, 0]
        for x in range(1, n_shell):
            total = total + p1r_v[i, x]
        summed.append(total)
    width = 8 * own
    summed.append(jnp.zeros((LANES - width, LANES), f32))
    p2t_v[...] = jnp.concatenate(summed, axis=0).T
    per = cycles // n_band
    packed = p2t_v[pl.ds(0, n_band, stride=per), :]
    for q in range(1, per):
        packed = packed + roll(p2t_v[pl.ds(q, n_band, stride=per), :], q * width, 1)
    for d in range(n_band):
        p2s_v[d] = packed[d : d + 1]

    @pl.loop(1, n_band)
    def _(j):
        d = peer(n_band - j)
        pltpu.make_async_remote_copy(
            src_ref=p2s_v.at[d],
            dst_ref=p2r_v.at[band],
            send_sem=p2s_sem,
            recv_sem=p2r_sem,
            device_id={"band": d},
            device_id_type=MESH,
        ).start()

    p2r_v[band] = p2s_v[band]
    last = pltpu.make_async_remote_copy(
        src_ref=p2r_v.at[pl.ds(0, n_band - 1)],
        dst_ref=p2r_v.at[pl.ds(0, n_band - 1)],
        send_sem=p2s_sem,
        recv_sem=p2r_sem,
        device_id={"band": peer(1)},
        device_id_type=MESH,
    )
    last.wait_recv()
    got = jnp.concatenate(
        [p2r_v[d] for d in range(n_band)] + [jnp.zeros((LANES - n_band, LANES), f32)], axis=0
    ).T
    lane = lax.broadcasted_iota(jnp.int32, (8, LANES), 1)
    for q in range(per):
        field = jnp.zeros((8, LANES), f32)
        for i in range(own):
            block = got[(q * own + i) * 8 : (q * own + i) * 8 + 8]
            block = jnp.take_along_axis(block, lane // own, axis=1)
            field = jnp.where(lane % own == i, block, field)
        for f in range(3):
            at = f * 2 * per + 2 * q
            out[at : at + 2, :] = field[2 * f : 2 * f + 2]
    for i in range(own):
        all_orders(i).wait_send()
        all_bins(i).wait_send()
    last.wait_send()


def on_device(n_band, n_shell, modes, weight, legendre, plus, minus, window, lensing, source):
    f32, bf16 = jnp.float32, jnp.bfloat16
    own, cycles, degrees = legendre.shape
    shells, per, parts, orders = modes.shape
    rows = per * parts
    bins = n_shell
    vmem, smem, hbm = pltpu.VMEM, pltpu.SMEM, pl.ANY
    dma = pltpu.SemaphoreType.DMA
    maps = pl.pallas_call(
        functools.partial(kernel, n_band, n_shell),
        out_shape=jax.ShapeDtypeStruct((3 * rows, orders), f32),
        in_specs=[
            pl.BlockSpec(memory_space=hbm),
            pl.BlockSpec(memory_space=smem),
            pl.BlockSpec(memory_space=hbm),
            pl.BlockSpec(memory_space=hbm),
            pl.BlockSpec(memory_space=hbm),
            pl.BlockSpec(memory_space=hbm),
            pl.BlockSpec(memory_space=vmem),
            pl.BlockSpec(memory_space=smem),
        ],
        out_specs=pl.BlockSpec(memory_space=vmem),
        scratch_shapes=[
            vmem((shells * rows, orders), f32),
            vmem((orders * rows, shells), f32),
            vmem((orders * rows, shells), f32),
            vmem((own, cycles, degrees), f32),
            vmem((own, 4 * cycles, degrees), bf16),
            vmem((shells, degrees), f32),
            vmem((bins, shells, LANES), f32),
            vmem((8, degrees), f32),
            vmem((2 * shells, 2 * cycles), bf16),
            vmem((2 * shells, cycles), bf16),
            vmem((2 * shells, TILE), f32),
            vmem((2 * shells, TILE), f32),
            vmem((8 * bins, degrees), bf16),
            vmem((own, n_shell, 8, LANES), f32),
            vmem((own, n_shell, 8, LANES), f32),
            vmem((cycles, LANES), f32),
            vmem((n_band, 1, LANES), f32),
            vmem((n_band, 1, LANES), f32),
            dma((2,)),
            dma((own,)),
            dma((own,)),
            dma((own,)),
            dma((own,)),
            dma((own,)),
            dma((own,)),
            dma((own,)),
            dma,
            dma,
        ],
        compiler_params=pltpu.CompilerParams(
            collective_id=0, has_side_effects=True, vmem_limit_bytes=60 * 2**20
        ),
    )(
        modes.reshape(shells * rows, orders),
        weight,
        legendre,
        plus,
        minus,
        window,
        lensing.reshape(1, shells),
        source,
    )
    return maps.reshape(1, 3, per, parts, orders)


def solution(mesh):
    in_specs = (
        P(("cosmo", "shell"), "band", None, None),
        P("band"),
        P("band", None, None),
        P("band", None, None),
        P("band", None, None),
        P("shell", None),
        P(("cosmo", "shell")),
        P("cosmo"),
    )
    out_specs = P(("cosmo", "shell"), None, "band", None, None)
    return jax.shard_map(
        functools.partial(on_device, mesh.shape["band"], mesh.shape["shell"]),
        mesh=mesh,
        in_specs=in_specs,
        out_specs=out_specs,
        check_vma=False,
    )
```

```python
import functools

import jax
import jax.numpy as jnp
from jax import lax
from jax.experimental import pallas as pl
from jax.experimental.pallas import tpu as pltpu
from jax.sharding import PartitionSpec as P

MESH = pl.DeviceIdType.MESH
LANES = 128
TILE = 512


def roll(x, shift, axis):
    return pltpu.roll(x, shift, axis)


def kernel(
    n_band,
    n_shell,
    modes,
    weight,
    legendre,
    plus,
    minus,
    window,
    lensing,
    source,
    out,
    modes_v,
    send_v,
    recv_v,
    leg_v,
    tab_v,
    win_v,
    eff_v,
    fac_v,
    a_v,
    x_v,
    h0_v,
    h1_v,
    w_v,
    m_v,
    p1s_v,
    p1r_v,
    p2t_v,
    p2s_v,
    p2r_v,
    near_sem,
    in_sem,
    leg_sem,
    plus_sem,
    minus_sem,
    send_sem,
    recv_sem,
    p1s_sem,
    p1r_sem,
    p2s_sem,
    p2r_sem,
):
    f32, bf16 = jnp.float32, jnp.bfloat16
    band, shell = lax.axis_index("band"), lax.axis_index("shell")
    chips = n_band // 2
    chip, core = band // 2, band % 2
    own = legendre.shape[0]
    cycles = legendre.shape[1]
    degrees = legendre.shape[2]
    shells = window.shape[0]
    bins = n_shell
    rows = 2 * (cycles // n_band)

    def peer(j):
        k = j // 2
        step = ((k + 1) // 2) * (2 * (k % 2) - 1)
        return 2 * ((chip + step + chips) % chips) + (core + j) % 2

    get_modes = pltpu.make_async_copy(modes, modes_v, in_sem.at[0])
    get_window = pltpu.make_async_copy(window, win_v, in_sem.at[1])
    get_modes.start()

    def along(step, to):
        return {"band": 2 * ((chip + step + chips) % chips) + to}

    barrier = pltpu.get_barrier_semaphore()
    others = [{"shell": (shell + dx) % n_shell} for dx in range(1, n_shell)]
    first = [along(1, core), along(-1, core), along(0, 1 - core)]
    for d in first + others:
        pl.semaphore_signal(barrier, inc=1, device_id=d, device_id_type=MESH)
    pl.semaphore_wait(barrier, len(first + others))

    def tell(level):
        for sign in (1, -1):
            pl.semaphore_signal(
                near_sem.at[level],
                inc=1,
                device_id=along(sign * 2**level, core),
                device_id_type=MESH,
            )

    tell(0)

    def get_legendre(i):
        return pltpu.make_async_copy(legendre.at[i], leg_v.at[i], leg_sem.at[i])

    def get_plus(i):
        at = pl.ds(2 * cycles, cycles)
        return pltpu.make_async_copy(plus.at[i], tab_v.at[i, at], plus_sem.at[i])

    def get_minus(i):
        at = pl.ds(3 * cycles, cycles)
        return pltpu.make_async_copy(minus.at[i], tab_v.at[i, at], minus_sem.at[i])

    for i in range(own):
        get_legendre(i).start()
    get_window.start()
    for i in range(own):
        get_plus(i).start()
        get_minus(i).start()

    get_modes.wait()
    for k in range(rows):
        block = modes_v[pl.ds(k, shells, stride=rows), :] * weight[k // 2]
        send_v[pl.ds(k, LANES, stride=rows), :] = block.T

    def order_copy(i, d):
        return pltpu.make_async_remote_copy(
            src_ref=send_v.at[pl.ds(pl.multiple_of((own * d + i) * rows, rows), rows)],
            dst_ref=recv_v.at[pl.ds(pl.multiple_of((i * n_band + band) * rows, rows), rows)],
            send_sem=send_sem.at[i],
            recv_sem=recv_sem.at[i],
            device_id={"band": d},
            device_id_type=MESH,
        )

    def send(begin, end, orders):
        @pl.loop(begin, end)
        def _(j):
            d = peer(j)
            for i in orders:
                order_copy(i, d).start()

    levels = chips.bit_length() - 2
    every = range(own)
    reach = 2
    for level in range(levels):
        pl.semaphore_wait(near_sem.at[level], 2)
        if level + 1 < levels:
            tell(level + 1)
        else:
            pl.semaphore_signal(
                near_sem.at[levels], inc=1, device_id=along(0, 1 - core), device_id_type=MESH
            )
            break
        begin, reach = reach, 2 ** (level + 2) * 2 - 2
        send(1 if level == 0 else begin, reach, every)
    pl.semaphore_wait(near_sem.at[levels], 1)
    for i in every:
        send(reach, n_band, [i])
        recv_v[pl.ds(pl.multiple_of((i * n_band + band) * rows, rows), rows), :] = send_v[
            pl.ds(pl.multiple_of((own * band + i) * rows, rows), rows), :
        ]

    def all_orders(i):
        n = (n_band - 1) * rows
        at = pl.ds(pl.multiple_of(i * n_band * rows, rows), n)
        return pltpu.make_async_remote_copy(
            src_ref=recv_v.at[at],
            dst_ref=recv_v.at[at],
            send_sem=send_sem.at[i],
            recv_sem=recv_sem.at[i],
            device_id={"band": peer(1)},
            device_id_type=MESH,
        )

    spread = jnp.broadcast_to(lensing[0:1, :], (LANES, LANES)).T
    shell_id = shell * shells + lax.broadcasted_iota(jnp.int32, (shells, LANES), 0)
    for b in range(bins):
        at = jnp.full((shells, LANES), source[b], jnp.int32)
        eff_v[b] = spread * jnp.maximum(at - shell_id, 0).astype(f32) / (at + 1).astype(f32)

    sub = lax.broadcasted_iota(jnp.int32, (8, LANES), 0)
    even = sub % 2 == 0

    @pl.loop(0, degrees // LANES)
    def _(k):
        at = pl.multiple_of(k * LANES, LANES)
        degree = (at + lax.broadcasted_iota(jnp.int32, (8, LANES), 1)).astype(f32)
        ratio = jnp.where(
            degree >= 2.0,
            jnp.sqrt((degree + 2.0) * (degree - 1.0) / jnp.maximum(degree * (degree + 1.0), 1.0)),
            0.0,
        )
        fac_v[0:8, pl.ds(at, LANES)] = -ratio
        fac_v[8:16, pl.ds(at, LANES)] = jnp.where(even, ratio, -ratio)

    @pl.loop(0, own)
    def _(i):
        get_legendre(i).wait()

        @pl.loop(0, cycles // 16)
        def _(k):
            at = pl.ds(pl.multiple_of(k * 16, 16), 16)
            value = leg_v[i, at, :]
            high = value.astype(bf16)
            tab_v[i, at, :] = high
            at = pl.ds(pl.multiple_of(cycles + k * 16, 16), 16)
            tab_v[i, at, :] = (value - high.astype(f32)).astype(bf16)

    get_window.wait()

    def transform(i, t, h_v):
        table = tab_v[i, 0 : 2 * cycles, pl.ds(pl.multiple_of(t * TILE, TILE), TILE)]
        h_v[...] = jnp.dot(a_v[...], table, preferred_element_type=f32) + jnp.dot(
            x_v[...], table[:cycles], preferred_element_type=f32
        )

    def merge(x, y, s):
        clear = (sub & s) == 0
        if s == 4:
            return jnp.where(clear, x, y) + roll(jnp.where(clear, y, x), 4, 0)
        return jnp.where(clear, x, y) + jnp.where(clear, roll(x, 8 - s, 0), roll(y, s, 0))

    def bin_sums(t, h_v):
        for k in range(TILE // LANES):
            lanes = pl.ds(pl.multiple_of(t * TILE + k * LANES, LANES), LANES)
            sums = [[None, None] for _ in range(bins)]
            for g in range(shells // 8):
                at = slice(8 * g, 8 * g + 8)
                w = win_v[at, lanes]
                for c in range(2):
                    h = h_v[c * shells + 8 * g : c * shells + 8 * g + 8, k * LANES : (k + 1) * LANES]
                    hw = h * w
                    for b in range(bins):
                        term = hw * eff_v[b, at, :]
                        sums[b][c] = term if g == 0 else sums[b][c] + term
            z = [[merge(sums[b][c], sums[b + 2][c], 4) for c in range(2)] for b in range(2)]
            z = [merge(z[0][c], z[1][c], 2) for c in range(2)]
            z = merge(z[0], z[1], 1)
            low = z - z.astype(bf16).astype(f32)
            turned = jnp.where(even, roll(z, 7, 0), roll(z, 1, 0))
            w_v[:, lanes] = jnp.concatenate(
                [z, low, z * fac_v[0:8, lanes], turned * fac_v[8:16, lanes]], axis=0
            ).astype(bf16)

    def products(i, t):
        at = pl.ds(pl.multiple_of(t * 2 * TILE, 2 * TILE), 2 * TILE)
        return lax.dot_general(
            tab_v[i, :, at], w_v[:, at], (((1,), (1,)), ((), ())), preferred_element_type=f32
        )

    pairs = degrees // (2 * TILE)

    def pair(i, t):
        transform(i, 2 * t + 1, h1_v)
        bin_sums(2 * t, h0_v)
        if not isinstance(t, int) or t < pairs - 1:
            transform(i, 2 * t + 2, h0_v)
        bin_sums(2 * t + 1, h1_v)

    @pl.loop(0, own)
    def _(i):
        all_orders(i).wait_recv()
        for c in range(2):
            x = recv_v[pl.ds(i * n_band * rows + c, cycles, stride=2), :].T
            high = x.astype(bf16)
            at = slice(c * shells, (c + 1) * shells)
            a_v[at, :cycles] = high
            a_v[at, cycles:] = high
            x_v[at, :] = (x - high.astype(f32)).astype(bf16)

        get_plus(i).wait()
        get_minus(i).wait()
        transform(i, 0, h0_v)
        pair(i, 0)
        m_v[...] = jnp.zeros_like(m_v)

        @pl.loop(1, pairs - 1)
        def _(t):
            m_v[...] += products(i, t - 1)
            pair(i, t)

        m_v[...] += products(i, pairs - 2)
        pair(i, pairs - 1)
        maps = (m_v[...] + products(i, pairs - 1)).T
        field = [maps[:, q * cycles : (q + 1) * cycles] for q in range(4)]
        kappa = field[0][0:8] + field[0][8:16] + field[1][0:8]
        p, m = field[2][16:24], field[3][24:32]
        for b in range(bins):
            k0, p0, m0 = (
                x if n % 8 == 0 else roll(x, n % 8, 0)
                for x, n in ((kappa, 8 - 2 * b), (p, 10 - 2 * b), (m, 12 - 2 * b))
            )
            p1s_v[i, b] = jnp.where(sub < 2, k0, jnp.where(sub < 4, p0, m0))
        for dx in range(1, n_shell):
            d = (shell + dx) % n_shell
            pltpu.make_async_remote_copy(
                src_ref=p1s_v.at[i, d],
                dst_ref=p1r_v.at[i, shell],
                send_sem=p1s_sem.at[i],
                recv_sem=p1r_sem.at[i],
                device_id={"shell": d},
                device_id_type=MESH,
            ).start()
        p1r_v[i, shell] = p1s_v[i, shell]

    def all_bins(i):
        return pltpu.make_async_remote_copy(
            src_ref=p1r_v.at[i, pl.ds(0, n_shell - 1)],
            dst_ref=p1r_v.at[i, pl.ds(0, n_shell - 1)],
            send_sem=p1s_sem.at[i],
            recv_sem=p1r_sem.at[i],
            device_id={"shell": (shell + 1) % n_shell},
            device_id_type=MESH,
        )

    summed = []
    for i in range(own):
        all_bins(i).wait_recv()
        total = p1r_v[i, 0]
        for x in range(1, n_shell):
            total = total + p1r_v[i, x]
        summed.append(total)
    width = 8 * own
    summed.append(jnp.zeros((LANES - width, LANES), f32))
    p2t_v[...] = jnp.concatenate(summed, axis=0).T
    per = cycles // n_band
    packed = p2t_v[pl.ds(0, n_band, stride=per), :]
    for q in range(1, per):
        packed = packed + roll(p2t_v[pl.ds(q, n_band, stride=per), :], q * width, 1)
    for d in range(n_band):
        p2s_v[d] = packed[d : d + 1]

    @pl.loop(1, n_band)
    def _(j):
        d = peer(n_band - j)
        pltpu.make_async_remote_copy(
            src_ref=p2s_v.at[d],
            dst_ref=p2r_v.at[band],
            send_sem=p2s_sem,
            recv_sem=p2r_sem,
            device_id={"band": d},
            device_id_type=MESH,
        ).start()

    p2r_v[band] = p2s_v[band]
    last = pltpu.make_async_remote_copy(
        src_ref=p2r_v.at[pl.ds(0, n_band - 1)],
        dst_ref=p2r_v.at[pl.ds(0, n_band - 1)],
        send_sem=p2s_sem,
        recv_sem=p2r_sem,
        device_id={"band": peer(1)},
        device_id_type=MESH,
    )
    last.wait_recv()
    got = jnp.concatenate(
        [p2r_v[d] for d in range(n_band)] + [jnp.zeros((LANES - n_band, LANES), f32)], axis=0
    ).T
    lane = lax.broadcasted_iota(jnp.int32, (8, LANES), 1)
    for q in range(per):
        field = jnp.zeros((8, LANES), f32)
        for i in range(own):
            block = got[(q * own + i) * 8 : (q * own + i) * 8 + 8]
            block = jnp.take_along_axis(block, lane // own, axis=1)
            field = jnp.where(lane % own == i, block, field)
        for f in range(3):
            at = f * 2 * per + 2 * q
            out[at : at + 2, :] = field[2 * f : 2 * f + 2]
    for i in range(own):
        all_orders(i).wait_send()
        all_bins(i).wait_send()
    last.wait_send()


def on_device(n_band, n_shell, modes, weight, legendre, plus, minus, window, lensing, source):
    f32, bf16 = jnp.float32, jnp.bfloat16
    own, cycles, degrees = legendre.shape
    shells, per, parts, orders = modes.shape
    rows = per * parts
    bins = n_shell
    vmem, smem, hbm = pltpu.VMEM, pltpu.SMEM, pl.ANY
    dma = pltpu.SemaphoreType.DMA
    maps = pl.pallas_call(
        functools.partial(kernel, n_band, n_shell),
        out_shape=jax.ShapeDtypeStruct((3 * rows, orders), f32),
        in_specs=[
            pl.BlockSpec(memory_space=hbm),
            pl.BlockSpec(memory_space=smem),
            pl.BlockSpec(memory_space=hbm),
            pl.BlockSpec(memory_space=hbm),
            pl.BlockSpec(memory_space=hbm),
            pl.BlockSpec(memory_space=hbm),
            pl.BlockSpec(memory_space=vmem),
            pl.BlockSpec(memory_space=smem),
        ],
        out_specs=pl.BlockSpec(memory_space=vmem),
        scratch_shapes=[
            vmem((shells * rows, orders), f32),
            vmem((orders * rows, shells), f32),
            vmem((orders * rows, shells), f32),
            vmem((own, cycles, degrees), f32),
            vmem((own, 4 * cycles, degrees), bf16),
            vmem((shells, degrees), f32),
            vmem((bins, shells, LANES), f32),
            vmem((16, degrees), f32),
            vmem((2 * shells, 2 * cycles), bf16),
            vmem((2 * shells, cycles), bf16),
            vmem((2 * shells, TILE), f32),
            vmem((2 * shells, TILE), f32),
            vmem((8 * bins, degrees), bf16),
            vmem((4 * cycles, 8 * bins), f32),
            vmem((own, n_shell, 8, LANES), f32),
            vmem((own, n_shell, 8, LANES), f32),
            vmem((cycles, LANES), f32),
            vmem((n_band, 1, LANES), f32),
            vmem((n_band, 1, LANES), f32),
            pltpu.SemaphoreType.REGULAR((n_band.bit_length() - 2,)),
            dma((2,)),
            dma((own,)),
            dma((own,)),
            dma((own,)),
            dma((own,)),
            dma((own,)),
            dma((own,)),
            dma((own,)),
            dma,
            dma,
        ],
        compiler_params=pltpu.CompilerParams(
            collective_id=0, has_side_effects=True, vmem_limit_bytes=60 * 2**20
        ),
    )(
        modes.reshape(shells * rows, orders),
        weight,
        legendre,
        plus,
        minus,
        window,
        lensing.reshape(1, shells),
        source,
    )
    return maps.reshape(1, 3, per, parts, orders)


def solution(mesh):
    in_specs = (
        P(("cosmo", "shell"), "band", None, None),
        P("band"),
        P("band", None, None),
        P("band", None, None),
        P("band", None, None),
        P("shell", None),
        P(("cosmo", "shell")),
        P("cosmo"),
    )
    out_specs = P(("cosmo", "shell"), None, "band", None, None)
    return jax.shard_map(
        functools.partial(on_device, mesh.shape["band"], mesh.shape["shell"]),
        mesh=mesh,
        in_specs=in_specs,
        out_specs=out_specs,
        check_vma=False,
    )
```

```python
import functools

import jax
import jax.numpy as jnp
from jax import lax
from jax.experimental import pallas as pl
from jax.experimental.pallas import tpu as pltpu
from jax.sharding import PartitionSpec as P

MESH = pl.DeviceIdType.MESH
LANES = 128
TILE = 512


def roll(x, shift, axis):
    return pltpu.roll(x, shift, axis)


def kernel(
    n_band,
    n_shell,
    modes,
    weight,
    legendre,
    plus,
    minus,
    window,
    lensing,
    source,
    out,
    weight_v,
    lensing_v,
    source_v,
    modes_v,
    send_v,
    recv_v,
    leg_v,
    tab_v,
    win_v,
    eff_v,
    fac_v,
    a_v,
    x_v,
    h0_v,
    h1_v,
    w_v,
    m_v,
    p1s_v,
    p1r_v,
    p2t_v,
    p2s_v,
    p2r_v,
    near_sem,
    in_sem,
    leg_sem,
    plus_sem,
    minus_sem,
    send_sem,
    recv_sem,
    p1s_sem,
    p1r_sem,
    p2s_sem,
    p2r_sem,
):
    f32, bf16 = jnp.float32, jnp.bfloat16
    band, shell = lax.axis_index("band"), lax.axis_index("shell")
    chips = n_band // 2
    chip, core = band // 2, band % 2
    own = legendre.shape[0]
    cycles = legendre.shape[1]
    degrees = legendre.shape[2]
    shells = window.shape[0]
    bins = n_shell
    rows = 2 * (cycles // n_band)

    def peer(j):
        k = j // 2
        step = ((k + 1) // 2) * (2 * (k % 2) - 1)
        return 2 * ((chip + step + chips) % chips) + (core + j) % 2

    get_modes = pltpu.make_async_copy(modes, modes_v, in_sem.at[0])
    get_window = pltpu.make_async_copy(window, win_v, in_sem.at[1])
    get_modes.start()
    get_small = [
        pltpu.make_async_copy(x, y, in_sem.at[2 + k])
        for k, (x, y) in enumerate(((weight, weight_v), (lensing, lensing_v), (source, source_v)))
    ]
    for copy in get_small:
        copy.start()

    near = chips // 4
    reach = 4 * near + 2

    barrier = pltpu.get_barrier_semaphore()

    @pl.loop(0, reach - 1)
    def _(j):
        pl.semaphore_signal(
            barrier, inc=1, device_id={"band": peer(reach - 1 - j)}, device_id_type=MESH
        )

    for dx in range(1, n_shell):
        pl.semaphore_signal(
            barrier, inc=1, device_id={"shell": (shell + dx) % n_shell}, device_id_type=MESH
        )
    pl.semaphore_wait(barrier, reach - 1 + n_shell - 1)

    for step in (near, -near):
        pl.semaphore_signal(
            near_sem,
            inc=1,
            device_id={"band": 2 * ((chip + step + chips) % chips) + core},
            device_id_type=MESH,
        )

    def get_legendre(i):
        return pltpu.make_async_copy(legendre.at[i], leg_v.at[i], leg_sem.at[i])

    def get_plus(i):
        at = pl.ds(2 * cycles, cycles)
        return pltpu.make_async_copy(plus.at[i], tab_v.at[i, at], plus_sem.at[i])

    def get_minus(i):
        at = pl.ds(3 * cycles, cycles)
        return pltpu.make_async_copy(minus.at[i], tab_v.at[i, at], minus_sem.at[i])

    for i in range(own):
        get_legendre(i).start()
    get_window.start()
    for i in range(own):
        get_plus(i).start()
        get_minus(i).start()

    get_modes.wait()
    for copy in get_small:
        copy.wait()
    for k in range(rows):
        scale = jnp.broadcast_to(weight_v[0:1, k // 2 : k // 2 + 1], (shells, LANES))
        block = modes_v[pl.ds(k, shells, stride=rows), :] * scale
        send_v[pl.ds(k, LANES, stride=rows), :] = block.T

    def order_copy(i, d):
        return pltpu.make_async_remote_copy(
            src_ref=send_v.at[pl.ds(pl.multiple_of((own * d + i) * rows, rows), rows)],
            dst_ref=recv_v.at[pl.ds(pl.multiple_of((i * n_band + band) * rows, rows), rows)],
            send_sem=send_sem.at[i],
            recv_sem=recv_sem.at[i],
            device_id={"band": d},
            device_id_type=MESH,
        )

    def send(begin, end, orders):
        @pl.loop(0, end - begin)
        def _(k):
            d = peer(end - 1 - k)
            for i in orders:
                order_copy(i, d).start()

    every = range(own)
    early = own // 2
    send(1, reach, range(early))
    pl.semaphore_wait(near_sem, 2)
    for i in every:
        send(reach if i < early else 1, n_band, [i])
    for i in every:
        recv_v[pl.ds(pl.multiple_of((i * n_band + band) * rows, rows), rows), :] = send_v[
            pl.ds(pl.multiple_of((own * band + i) * rows, rows), rows), :
        ]

    def all_orders(i):
        n = (n_band - 1) * rows
        at = pl.ds(pl.multiple_of(i * n_band * rows, rows), n)
        return pltpu.make_async_remote_copy(
            src_ref=recv_v.at[at],
            dst_ref=recv_v.at[at],
            send_sem=send_sem.at[i],
            recv_sem=recv_sem.at[i],
            device_id={"band": peer(1)},
            device_id_type=MESH,
        )

    spread = jnp.broadcast_to(lensing_v[0:1, :], (LANES, LANES)).T
    shell_id = shell * shells + lax.broadcasted_iota(jnp.int32, (shells, LANES), 0)
    for b in range(bins):
        at = jnp.broadcast_to(source_v[0:1, b : b + 1], (shells, LANES))
        eff_v[b] = spread * jnp.maximum(at - shell_id, 0).astype(f32) / (at + 1).astype(f32)

    sub = lax.broadcasted_iota(jnp.int32, (8, LANES), 0)
    even = sub % 2 == 0

    @pl.loop(0, degrees // LANES)
    def _(k):
        at = pl.multiple_of(k * LANES, LANES)
        degree = (at + lax.broadcasted_iota(jnp.int32, (8, LANES), 1)).astype(f32)
        ratio = jnp.where(
            degree >= 2.0,
            jnp.sqrt((degree + 2.0) * (degree - 1.0) / jnp.maximum(degree * (degree + 1.0), 1.0)),
            0.0,
        )
        fac_v[0:8, pl.ds(at, LANES)] = -ratio
        fac_v[8:16, pl.ds(at, LANES)] = jnp.where(even, ratio, -ratio)

    @pl.loop(0, own)
    def _(i):
        get_legendre(i).wait()

        @pl.loop(0, cycles // 16)
        def _(k):
            at = pl.ds(pl.multiple_of(k * 16, 16), 16)
            value = leg_v[i, at, :]
            high = value.astype(bf16)
            tab_v[i, at, :] = high
            at = pl.ds(pl.multiple_of(cycles + k * 16, 16), 16)
            tab_v[i, at, :] = (value - high.astype(f32)).astype(bf16)

    get_window.wait()

    def transform(i, t, h_v):
        table = tab_v[i, 0 : 2 * cycles, pl.ds(pl.multiple_of(t * TILE, TILE), TILE)]
        h_v[...] = jnp.dot(a_v[...], table, preferred_element_type=f32) + jnp.dot(
            x_v[...], table[:cycles], preferred_element_type=f32
        )

    def merge(x, y, s):
        clear = (sub & s) == 0
        if s == 4:
            return jnp.where(clear, x, y) + roll(jnp.where(clear, y, x), 4, 0)
        return jnp.where(clear, x, y) + jnp.where(clear, roll(x, 8 - s, 0), roll(y, s, 0))

    def bin_sums(t, h_v):
        for k in range(TILE // LANES):
            lanes = pl.ds(pl.multiple_of(t * TILE + k * LANES, LANES), LANES)
            sums = [[None, None] for _ in range(bins)]
            for g in range(shells // 8):
                at = slice(8 * g, 8 * g + 8)
                w = win_v[at, lanes]
                for c in range(2):
                    h = h_v[c * shells + 8 * g : c * shells + 8 * g + 8, k * LANES : (k + 1) * LANES]
                    hw = h * w
                    for b in range(bins):
                        term = hw * eff_v[b, at, :]
                        sums[b][c] = term if g == 0 else sums[b][c] + term
            z = [[merge(sums[b][c], sums[b + 2][c], 4) for c in range(2)] for b in range(2)]
            z = [merge(z[0][c], z[1][c], 2) for c in range(2)]
            z = merge(z[0], z[1], 1)
            low = z - z.astype(bf16).astype(f32)
            turned = jnp.where(even, roll(z, 7, 0), roll(z, 1, 0))
            w_v[:, lanes] = jnp.concatenate(
                [z, low, z * fac_v[0:8, lanes], turned * fac_v[8:16, lanes]], axis=0
            ).astype(bf16)

    def products(i, t):
        at = pl.ds(pl.multiple_of(t * 2 * TILE, 2 * TILE), 2 * TILE)
        return lax.dot_general(
            tab_v[i, :, at], w_v[:, at], (((1,), (1,)), ((), ())), preferred_element_type=f32
        )

    pairs = degrees // (2 * TILE)

    def pair(i, t):
        transform(i, 2 * t + 1, h1_v)
        bin_sums(2 * t, h0_v)
        if not isinstance(t, int) or t < pairs - 1:
            transform(i, 2 * t + 2, h0_v)
        bin_sums(2 * t + 1, h1_v)

    @pl.loop(0, own)
    def _(i):
        all_orders(i).wait_recv()
        for c in range(2):
            x = recv_v[pl.ds(i * n_band * rows + c, cycles, stride=2), :].T
            high = x.astype(bf16)
            at = slice(c * shells, (c + 1) * shells)
            a_v[at, :cycles] = high
            a_v[at, cycles:] = high
            x_v[at, :] = (x - high.astype(f32)).astype(bf16)

        get_plus(i).wait()
        get_minus(i).wait()
        transform(i, 0, h0_v)
        pair(i, 0)
        m_v[...] = jnp.zeros_like(m_v)

        @pl.loop(1, pairs - 1)
        def _(t):
            m_v[...] += products(i, t - 1)
            pair(i, t)

        m_v[...] += products(i, pairs - 2)
        pair(i, pairs - 1)
        maps = (m_v[...] + products(i, pairs - 1)).T
        field = [maps[:, q * cycles : (q + 1) * cycles] for q in range(4)]
        kappa = field[0][0:8] + field[0][8:16] + field[1][0:8]
        p, m = field[2][16:24], field[3][24:32]
        for b in range(bins):
            k0, p0, m0 = (
                x if n % 8 == 0 else roll(x, n % 8, 0)
                for x, n in ((kappa, 8 - 2 * b), (p, 10 - 2 * b), (m, 12 - 2 * b))
            )
            p1s_v[i, b] = jnp.where(sub < 2, k0, jnp.where(sub < 4, p0, m0))
        for dx in range(1, n_shell):
            d = (shell + dx) % n_shell
            pltpu.make_async_remote_copy(
                src_ref=p1s_v.at[i, d],
                dst_ref=p1r_v.at[i, shell],
                send_sem=p1s_sem.at[i],
                recv_sem=p1r_sem.at[i],
                device_id={"shell": d},
                device_id_type=MESH,
            ).start()
        p1r_v[i, shell] = p1s_v[i, shell]

    def all_bins(i):
        return pltpu.make_async_remote_copy(
            src_ref=p1r_v.at[i, pl.ds(0, n_shell - 1)],
            dst_ref=p1r_v.at[i, pl.ds(0, n_shell - 1)],
            send_sem=p1s_sem.at[i],
            recv_sem=p1r_sem.at[i],
            device_id={"shell": (shell + 1) % n_shell},
            device_id_type=MESH,
        )

    summed = []
    for i in range(own):
        all_bins(i).wait_recv()
        total = p1r_v[i, 0]
        for x in range(1, n_shell):
            total = total + p1r_v[i, x]
        summed.append(total)
    width = 8 * own
    summed.append(jnp.zeros((LANES - width, LANES), f32))
    p2t_v[...] = jnp.concatenate(summed, axis=0).T
    per = cycles // n_band
    packed = p2t_v[pl.ds(0, n_band, stride=per), :]
    for q in range(1, per):
        packed = packed + roll(p2t_v[pl.ds(q, n_band, stride=per), :], q * width, 1)
    for d in range(n_band):
        p2s_v[d] = packed[d : d + 1]

    @pl.loop(1, n_band)
    def _(j):
        d = peer(n_band - j)
        pltpu.make_async_remote_copy(
            src_ref=p2s_v.at[d],
            dst_ref=p2r_v.at[band],
            send_sem=p2s_sem,
            recv_sem=p2r_sem,
            device_id={"band": d},
            device_id_type=MESH,
        ).start()

    p2r_v[band] = p2s_v[band]
    last = pltpu.make_async_remote_copy(
        src_ref=p2r_v.at[pl.ds(0, n_band - 1)],
        dst_ref=p2r_v.at[pl.ds(0, n_band - 1)],
        send_sem=p2s_sem,
        recv_sem=p2r_sem,
        device_id={"band": peer(1)},
        device_id_type=MESH,
    )
    last.wait_recv()
    got = jnp.concatenate(
        [p2r_v[d] for d in range(n_band)] + [jnp.zeros((LANES - n_band, LANES), f32)], axis=0
    ).T
    lane = lax.broadcasted_iota(jnp.int32, (8, LANES), 1)
    for q in range(per):
        field = jnp.zeros((8, LANES), f32)
        for i in range(own):
            block = got[(q * own + i) * 8 : (q * own + i) * 8 + 8]
            block = jnp.take_along_axis(block, lane // own, axis=1)
            field = jnp.where(lane % own == i, block, field)
        for f in range(3):
            at = f * 2 * per + 2 * q
            out[at : at + 2, :] = field[2 * f : 2 * f + 2]
    for i in range(own):
        all_orders(i).wait_send()
        all_bins(i).wait_send()
    last.wait_send()


def on_device(n_band, n_shell, modes, weight, legendre, plus, minus, window, lensing, source):
    f32, bf16 = jnp.float32, jnp.bfloat16
    own, cycles, degrees = legendre.shape
    shells, per, parts, orders = modes.shape
    rows = per * parts
    bins = n_shell
    vmem, hbm = pltpu.VMEM, pl.ANY
    dma = pltpu.SemaphoreType.DMA
    maps = pl.pallas_call(
        functools.partial(kernel, n_band, n_shell),
        out_shape=vmem((3 * rows, orders), f32),
        in_specs=[pl.BlockSpec(memory_space=hbm)] * 8,
        out_specs=pl.BlockSpec(memory_space=vmem),
        scratch_shapes=[
            vmem((1, per), f32),
            vmem((1, shells), f32),
            vmem((1, bins), jnp.int32),
            vmem((shells * rows, orders), f32),
            vmem((orders * rows, shells), f32),
            vmem((orders * rows, shells), f32),
            vmem((own, cycles, degrees), f32),
            vmem((own, 4 * cycles, degrees), bf16),
            vmem((shells, degrees), f32),
            vmem((bins, shells, LANES), f32),
            vmem((16, degrees), f32),
            vmem((2 * shells, 2 * cycles), bf16),
            vmem((2 * shells, cycles), bf16),
            vmem((2 * shells, TILE), f32),
            vmem((2 * shells, TILE), f32),
            vmem((8 * bins, degrees), bf16),
            vmem((4 * cycles, 8 * bins), f32),
            vmem((own, n_shell, 8, LANES), f32),
            vmem((own, n_shell, 8, LANES), f32),
            vmem((cycles, LANES), f32),
            vmem((n_band, 1, LANES), f32),
            vmem((n_band, 1, LANES), f32),
            pltpu.SemaphoreType.REGULAR,
            dma((5,)),
            dma((own,)),
            dma((own,)),
            dma((own,)),
            dma((own,)),
            dma((own,)),
            dma((own,)),
            dma((own,)),
            dma,
            dma,
        ],
        compiler_params=pltpu.CompilerParams(
            collective_id=0, has_side_effects=True, vmem_limit_bytes=60 * 2**20
        ),
    )(
        modes.reshape(shells * rows, orders),
        weight.reshape(1, per),
        legendre,
        plus,
        minus,
        window,
        lensing.reshape(1, shells),
        source.reshape(1, bins),
    )
    return maps.reshape(1, 3, per, parts, orders)


def solution(mesh):
    in_specs = (
        P(("cosmo", "shell"), "band", None, None),
        P("band"),
        P("band", None, None),
        P("band", None, None),
        P("band", None, None),
        P("shell", None),
        P(("cosmo", "shell")),
        P("cosmo"),
    )
    out_specs = P(("cosmo", "shell"), None, "band", None, None)
    return jax.shard_map(
        functools.partial(on_device, mesh.shape["band"], mesh.shape["shell"]),
        mesh=mesh,
        in_specs=in_specs,
        out_specs=out_specs,
        check_vma=False,
    )
```

```python
import functools

import jax
import jax.numpy as jnp
from jax import lax
from jax.experimental import pallas as pl
from jax.experimental.pallas import tpu as pltpu
from jax.sharding import PartitionSpec as P

MESH = pl.DeviceIdType.MESH
LANES = 128
TILE = 512


def roll(x, shift, axis):
    return pltpu.roll(x, shift, axis)


def kernel(
    n_band,
    n_shell,
    modes,
    weight,
    legendre,
    plus,
    minus,
    window,
    lensing,
    source,
    out,
    weight_v,
    lensing_v,
    source_v,
    modes_v,
    send_v,
    recv_v,
    leg_v,
    tab_v,
    win_v,
    eff_v,
    fac_v,
    a_v,
    x_v,
    h0_v,
    h1_v,
    w_v,
    m_v,
    p1s_v,
    p1r_v,
    p2t_v,
    p2s_v,
    p2r_v,
    near_sem,
    in_sem,
    leg_sem,
    plus_sem,
    minus_sem,
    send_sem,
    recv_sem,
    p1s_sem,
    p1r_sem,
    p2s_sem,
    p2r_sem,
):
    f32, bf16 = jnp.float32, jnp.bfloat16
    band, shell = lax.axis_index("band"), lax.axis_index("shell")
    chips = n_band // 2
    chip, core = band // 2, band % 2
    own = legendre.shape[0]
    cycles = legendre.shape[1]
    degrees = legendre.shape[2]
    shells = window.shape[0]
    bins = n_shell
    rows = 2 * (cycles // n_band)

    def peer(j):
        k = lax.div(j, 2)
        step = lax.div(k + 1, 2) * (2 * lax.rem(k, 2) - 1)
        return 2 * lax.rem(chip + step + chips, chips) + lax.rem(core + j, 2)

    get_modes = pltpu.make_async_copy(modes, modes_v, in_sem.at[0])
    get_window = pltpu.make_async_copy(window, win_v, in_sem.at[1])
    get_modes.start()
    get_small = [
        pltpu.make_async_copy(x, y, in_sem.at[2 + k])
        for k, (x, y) in enumerate(((weight, weight_v), (lensing, lensing_v), (source, source_v)))
    ]
    for copy in get_small:
        copy.start()

    near = chips // 4
    reach = 4 * near + 2

    barrier = pltpu.get_barrier_semaphore()

    @pl.loop(0, reach - 1)
    def _(j):
        pl.semaphore_signal(
            barrier, inc=1, device_id={"band": peer(reach - 1 - j)}, device_id_type=MESH
        )

    for dx in range(1, n_shell):
        pl.semaphore_signal(
            barrier, inc=1, device_id={"shell": (shell + dx) % n_shell}, device_id_type=MESH
        )
    pl.semaphore_wait(barrier, reach - 1 + n_shell - 1)

    for step in (near, -near):
        pl.semaphore_signal(
            near_sem,
            inc=1,
            device_id={"band": 2 * ((chip + step + chips) % chips) + core},
            device_id_type=MESH,
        )

    def get_legendre(i):
        return pltpu.make_async_copy(legendre.at[i], leg_v.at[i], leg_sem.at[i])

    def get_plus(i):
        at = pl.ds(2 * cycles, cycles)
        return pltpu.make_async_copy(plus.at[i], tab_v.at[i, at], plus_sem.at[i])

    def get_minus(i):
        at = pl.ds(3 * cycles, cycles)
        return pltpu.make_async_copy(minus.at[i], tab_v.at[i, at], minus_sem.at[i])

    for i in range(own):
        get_legendre(i).start()
    get_window.start()
    for i in range(own):
        get_plus(i).start()
        get_minus(i).start()

    get_modes.wait()
    for copy in get_small:
        copy.wait()
    per = rows // 2
    for r in range(per):
        scale = jnp.broadcast_to(weight_v[0:1, r : r + 1], (shells, LANES))
        for c in range(2):
            block = modes_v[pl.ds(2 * r + c, shells, stride=rows), :] * scale
            send_v[pl.ds(c * per + r, LANES, stride=rows), :] = block.T

    def order_copy(i, d, c=None):
        n, skip = (rows, 0) if c is None else (per, c * per)
        return pltpu.make_async_remote_copy(
            src_ref=send_v.at[pl.ds(pl.multiple_of((own * d + i) * rows + skip, n), n)],
            dst_ref=recv_v.at[pl.ds(pl.multiple_of((i * n_band + band) * rows + skip, n), n)],
            send_sem=send_sem.at[i],
            recv_sem=recv_sem.at[i if c is None else i + c],
            device_id={"band": d},
            device_id_type=MESH,
        )

    def send(begin, end, orders, c=None):
        @pl.loop(0, end - begin)
        def _(k):
            d = peer(end - 1 - k)
            for i in orders:
                order_copy(i, d, c).start()

    final = own - 1
    early = own // 2
    send(1, reach, range(early))
    pl.semaphore_wait(near_sem, 2)
    for i in range(final):
        send(reach if i < early else 1, n_band, [i])
    for c in range(2):
        send(1, n_band, [final], c)
    for i in range(own):
        recv_v[pl.ds(pl.multiple_of((i * n_band + band) * rows, rows), rows), :] = send_v[
            pl.ds(pl.multiple_of((own * band + i) * rows, rows), rows), :
        ]

    def all_orders(i, c=None):
        n = (n_band - 1) * (rows if c is None else per)
        at = pl.ds(pl.multiple_of(i * n_band * rows, rows), n)
        return pltpu.make_async_remote_copy(
            src_ref=recv_v.at[at],
            dst_ref=recv_v.at[at],
            send_sem=send_sem.at[i],
            recv_sem=recv_sem.at[i if c is None else i + c],
            device_id={"band": 2 * chip + 1 - core},
            device_id_type=MESH,
        )

    spread = jnp.broadcast_to(lensing_v[0:1, :], (LANES, LANES)).T
    shell_id = shell * shells + lax.broadcasted_iota(jnp.int32, (shells, LANES), 0)
    for b in range(bins):
        at = jnp.broadcast_to(source_v[0:1, b : b + 1], (shells, LANES))
        eff_v[b] = spread * jnp.maximum(at - shell_id, 0).astype(f32) / (at + 1).astype(f32)

    sub = lax.broadcasted_iota(jnp.int32, (8, LANES), 0)
    even = sub % 2 == 0

    @pl.loop(0, degrees // LANES)
    def _(k):
        at = pl.multiple_of(k * LANES, LANES)
        degree = (at + lax.broadcasted_iota(jnp.int32, (8, LANES), 1)).astype(f32)
        ratio = jnp.where(
            degree >= 2.0,
            jnp.sqrt((degree + 2.0) * (degree - 1.0) / jnp.maximum(degree * (degree + 1.0), 1.0)),
            0.0,
        )
        fac_v[0:8, pl.ds(at, LANES)] = -ratio
        fac_v[8:16, pl.ds(at, LANES)] = jnp.where(even, ratio, -ratio)

    @pl.loop(0, own)
    def _(i):
        get_legendre(i).wait()

        @pl.loop(0, cycles // 16)
        def _(k):
            at = pl.ds(pl.multiple_of(k * 16, 16), 16)
            value = leg_v[i, at, :]
            high = value.astype(bf16)
            tab_v[i, at, :] = high
            at = pl.ds(pl.multiple_of(cycles + k * 16, 16), 16)
            tab_v[i, at, :] = (value - high.astype(f32)).astype(bf16)

    get_window.wait()

    def transform(i, t, h_v, cs):
        table = tab_v[i, 0 : 2 * cycles, pl.ds(pl.multiple_of(t * TILE, TILE), TILE)]
        h = jnp.dot(a_v[...], table, preferred_element_type=f32)
        if len(cs) == 2:
            h = h + jnp.dot(x_v[...], table[:cycles], preferred_element_type=f32)
        h_v[...] = h

    def merge(x, y, s):
        clear = (sub & s) == 0
        if s == 4:
            return jnp.where(clear, x, y) + roll(jnp.where(clear, y, x), 4, 0)
        return jnp.where(clear, x, y) + jnp.where(clear, roll(x, 8 - s, 0), roll(y, s, 0))

    def bin_sums(t, h_v, cs):
        for k in range(TILE // LANES):
            lanes = pl.ds(pl.multiple_of(t * TILE + k * LANES, LANES), LANES)
            here = slice(k * LANES, (k + 1) * LANES)
            sums = [[None] * len(cs) for _ in range(bins)]
            for g in range(shells // 8):
                at = slice(8 * g, 8 * g + 8)
                after = slice(shells + 8 * g, shells + 8 * g + 8)
                w = win_v[at, lanes]
                hs = [h_v[at, here], h_v[after, here]]
                if len(cs) == 1:
                    hs = [hs[0] + hs[1]]
                for c, h in enumerate(hs):
                    hw = h * w
                    for b in range(bins):
                        term = hw * eff_v[b, at, :]
                        sums[b][c] = term if g == 0 else sums[b][c] + term
            z = [[merge(x, y, 4) for x, y in zip(sums[b], sums[b + 2])] for b in range(2)]
            z = [merge(x, y, 2) for x, y in zip(*z)]
            z = merge(z[0], z[-1], 1)
            low = z - z.astype(bf16).astype(f32)
            turned = jnp.where(even, roll(z, 7, 0), roll(z, 1, 0))
            w_v[:, lanes] = jnp.concatenate(
                [z, low, z * fac_v[0:8, lanes], turned * fac_v[8:16, lanes]], axis=0
            ).astype(bf16)

    def products(i, t):
        at = pl.ds(pl.multiple_of(t * 2 * TILE, 2 * TILE), 2 * TILE)
        return lax.dot_general(
            tab_v[i, :, at], w_v[:, at], (((1,), (1,)), ((), ())), preferred_element_type=f32
        )

    pairs = degrees // (2 * TILE)

    def pair(i, t, cs):
        transform(i, 2 * t + 1, h1_v, cs)
        bin_sums(2 * t, h0_v, cs)
        if not isinstance(t, int) or t < pairs - 1:
            transform(i, 2 * t + 2, h0_v, cs)
        bin_sums(2 * t + 1, h1_v, cs)

    def part_of(i, c, cs):
        tiles = []
        for q in range(n_band // 2):
            at = i * n_band * rows + 2 * rows * q
            if len(cs) == 1:
                at = at + c * per
                tiles.append(recv_v[pl.ds(at, per), :])
                tiles.append(recv_v[pl.ds(at + rows, per), :])
                continue
            at = pl.multiple_of(at, 2 * rows)
            x, y = recv_v[pl.ds(at, rows), :], recv_v[pl.ds(at + rows, rows), :]
            if c == 0:
                tiles.append(jnp.where(sub < per, x, roll(y, per, 0)))
            else:
                tiles.append(jnp.where(sub < per, roll(x, per, 0), y))
        return jnp.concatenate(tiles, axis=0).T

    def work(i, cs):
        for k, c in enumerate(cs):
            x = part_of(i, c, cs)
            high = x.astype(bf16)
            low = (x - high.astype(f32)).astype(bf16)
            at = slice(k * shells, (k + 1) * shells)
            a_v[at, :cycles] = high
            a_v[at, cycles:] = high
            if len(cs) == 2:
                x_v[at, :] = low
            else:
                a_v[shells:, :cycles] = low
                a_v[shells:, cycles:] = low
        transform(i, 0, h0_v, cs)
        pair(i, 0, cs)
        m_v[...] = jnp.zeros_like(m_v)

        @pl.loop(1, pairs - 1)
        def _(t):
            m_v[...] += products(i, t - 1)
            pair(i, t, cs)

        m_v[...] += products(i, pairs - 2)
        pair(i, pairs - 1, cs)
        maps = (m_v[...] + products(i, pairs - 1)).T
        field = [maps[:, q * cycles : (q + 1) * cycles] for q in range(4)]
        return field[0][0:8] + field[0][8:16] + field[1][0:8], field[2][16:24], field[3][24:32]

    def give(i, kappa, p, m):
        for b in range(bins):
            k0, p0, m0 = (
                x if n % 8 == 0 else roll(x, n % 8, 0)
                for x, n in ((kappa, 8 - 2 * b), (p, 10 - 2 * b), (m, 12 - 2 * b))
            )
            p1s_v[i, b] = jnp.where(sub < 2, k0, jnp.where(sub < 4, p0, m0))
        for dx in range(1, n_shell):
            d = (shell + dx) % n_shell
            pltpu.make_async_remote_copy(
                src_ref=p1s_v.at[i, d],
                dst_ref=p1r_v.at[i, shell],
                send_sem=p1s_sem.at[i],
                recv_sem=p1r_sem.at[i],
                device_id={"shell": d},
                device_id_type=MESH,
            ).start()
        p1r_v[i, shell] = p1s_v[i, shell]

    @pl.loop(0, final)
    def _(i):
        all_orders(i).wait_recv()
        get_plus(i).wait()
        get_minus(i).wait()
        give(i, *work(i, (0, 1)))

    get_plus(final).wait()
    get_minus(final).wait()
    all_orders(final, 0).wait_recv()
    real = work(final, (0,))
    all_orders(final, 1).wait_recv()
    imag = work(final, (1,))
    give(
        final,
        jnp.where(even, real[0], imag[0]),
        jnp.where(even, real[1], imag[1]),
        jnp.where(even, imag[2], real[2]),
    )

    def all_bins(i):
        return pltpu.make_async_remote_copy(
            src_ref=p1r_v.at[i, pl.ds(0, n_shell - 1)],
            dst_ref=p1r_v.at[i, pl.ds(0, n_shell - 1)],
            send_sem=p1s_sem.at[i],
            recv_sem=p1r_sem.at[i],
            device_id={"shell": (shell + 1) % n_shell},
            device_id_type=MESH,
        )

    summed = []
    for i in range(own):
        all_bins(i).wait_recv()
        total = p1r_v[i, 0]
        for x in range(1, n_shell):
            total = total + p1r_v[i, x]
        summed.append(total)
    width = 8 * own
    summed.append(jnp.zeros((LANES - width, LANES), f32))
    p2t_v[...] = jnp.concatenate(summed, axis=0).T
    packed = p2t_v[pl.ds(0, n_band, stride=per), :]
    for q in range(1, per):
        packed = packed + roll(p2t_v[pl.ds(q, n_band, stride=per), :], q * width, 1)
    for d in range(n_band):
        p2s_v[d] = packed[d : d + 1]

    @pl.loop(1, n_band)
    def _(j):
        d = peer(n_band - j)
        pltpu.make_async_remote_copy(
            src_ref=p2s_v.at[d],
            dst_ref=p2r_v.at[band],
            send_sem=p2s_sem,
            recv_sem=p2r_sem,
            device_id={"band": d},
            device_id_type=MESH,
        ).start()

    p2r_v[band] = p2s_v[band]
    last = pltpu.make_async_remote_copy(
        src_ref=p2r_v.at[pl.ds(0, n_band - 1)],
        dst_ref=p2r_v.at[pl.ds(0, n_band - 1)],
        send_sem=p2s_sem,
        recv_sem=p2r_sem,
        device_id={"band": 2 * chip + 1 - core},
        device_id_type=MESH,
    )
    last.wait_recv()
    got = jnp.concatenate(
        [p2r_v[d] for d in range(n_band)] + [jnp.zeros((LANES - n_band, LANES), f32)], axis=0
    ).T
    lane = lax.broadcasted_iota(jnp.int32, (8, LANES), 1)
    for q in range(per):
        field = jnp.zeros((8, LANES), f32)
        for i in range(own):
            block = got[(q * own + i) * 8 : (q * own + i) * 8 + 8]
            block = jnp.take_along_axis(block, lane // own, axis=1)
            field = jnp.where(lane % own == i, block, field)
        for f in range(3):
            at = f * 2 * per + 2 * q
            out[at : at + 2, :] = field[2 * f : 2 * f + 2]
    for i in range(own):
        all_orders(i).wait_send()
        all_bins(i).wait_send()
    last.wait_send()


def on_device(n_band, n_shell, modes, weight, legendre, plus, minus, window, lensing, source):
    f32, bf16 = jnp.float32, jnp.bfloat16
    own, cycles, degrees = legendre.shape
    shells, per, parts, orders = modes.shape
    rows = per * parts
    bins = n_shell
    vmem, hbm = pltpu.VMEM, pl.ANY
    dma = pltpu.SemaphoreType.DMA
    maps = pl.pallas_call(
        functools.partial(kernel, n_band, n_shell),
        out_shape=vmem((3 * rows, orders), f32),
        in_specs=[pl.BlockSpec(memory_space=hbm)] * 8,
        out_specs=pl.BlockSpec(memory_space=vmem),
        scratch_shapes=[
            vmem((1, per), f32),
            vmem((1, shells), f32),
            vmem((1, bins), jnp.int32),
            vmem((shells * rows, orders), f32),
            vmem((orders * rows, shells), f32),
            vmem((orders * rows, shells), f32),
            vmem((own, cycles, degrees), f32),
            vmem((own, 4 * cycles, degrees), bf16),
            vmem((shells, degrees), f32),
            vmem((bins, shells, LANES), f32),
            vmem((16, degrees), f32),
            vmem((2 * shells, 2 * cycles), bf16),
            vmem((2 * shells, cycles), bf16),
            vmem((2 * shells, TILE), f32),
            vmem((2 * shells, TILE), f32),
            vmem((8 * bins, degrees), bf16),
            vmem((4 * cycles, 8 * bins), f32),
            vmem((own, n_shell, 8, LANES), f32),
            vmem((own, n_shell, 8, LANES), f32),
            vmem((cycles, LANES), f32),
            vmem((n_band, 1, LANES), f32),
            vmem((n_band, 1, LANES), f32),
            pltpu.SemaphoreType.REGULAR,
            dma((5,)),
            dma((own,)),
            dma((own,)),
            dma((own,)),
            dma((own,)),
            dma((own + 1,)),
            dma((own,)),
            dma((own,)),
            dma,
            dma,
        ],
        compiler_params=pltpu.CompilerParams(
            collective_id=0, has_side_effects=True, vmem_limit_bytes=60 * 2**20
        ),
    )(
        modes.reshape(shells * rows, orders),
        weight.reshape(1, per),
        legendre,
        plus,
        minus,
        window,
        lensing.reshape(1, shells),
        source.reshape(1, bins),
    )
    return maps.reshape(1, 3, per, parts, orders)


def solution(mesh):
    in_specs = (
        P(("cosmo", "shell"), "band", None, None),
        P("band"),
        P("band", None, None),
        P("band", None, None),
        P("band", None, None),
        P("shell", None),
        P(("cosmo", "shell")),
        P("cosmo"),
    )
    out_specs = P(("cosmo", "shell"), None, "band", None, None)
    return jax.shard_map(
        functools.partial(on_device, mesh.shape["band"], mesh.shape["shell"]),
        mesh=mesh,
        in_specs=in_specs,
        out_specs=out_specs,
        check_vma=False,
    )
```

```python
import functools

import jax
import jax.numpy as jnp
from jax import lax
from jax.experimental import pallas as pl
from jax.experimental.pallas import tpu as pltpu
from jax.sharding import PartitionSpec as P

MESH = pl.DeviceIdType.MESH
LANES = 128
TILE = 512


def roll(x, shift, axis):
    return pltpu.roll(x, shift, axis)


def kernel(
    n_band,
    n_shell,
    modes,
    weight,
    legendre,
    plus,
    minus,
    window,
    lensing,
    source,
    out,
    weight_v,
    lensing_v,
    source_v,
    modes_v,
    send_v,
    recv_v,
    leg_v,
    tab_v,
    win_v,
    eff_v,
    fac_v,
    a_v,
    x_v,
    h0_v,
    h1_v,
    w_v,
    m_v,
    p1s_v,
    p1r_v,
    p2t_v,
    p2s_v,
    p2r_v,
    near_sem,
    in_sem,
    leg_sem,
    plus_sem,
    minus_sem,
    send_sem,
    recv_sem,
    p1s_sem,
    p1r_sem,
    p2s_sem,
    p2r_sem,
):
    f32, bf16 = jnp.float32, jnp.bfloat16
    band, shell = lax.axis_index("band"), lax.axis_index("shell")
    chips = n_band // 2
    chip, core = band // 2, band % 2
    own = legendre.shape[0]
    cycles = legendre.shape[1]
    degrees = legendre.shape[2]
    shells = window.shape[0]
    bins = n_shell
    rows = 2 * (cycles // n_band)

    def peer(j):
        k = lax.div(j, 2)
        step = lax.div(k + 1, 2) * (2 * lax.rem(k, 2) - 1)
        return 2 * lax.rem(chip + step + chips, chips) + lax.rem(core + j, 2)

    get_modes = pltpu.make_async_copy(modes, modes_v, in_sem.at[0])
    get_window = pltpu.make_async_copy(window, win_v, in_sem.at[1])
    get_modes.start()
    get_small = [
        pltpu.make_async_copy(x, y, in_sem.at[2 + k])
        for k, (x, y) in enumerate(((weight, weight_v), (lensing, lensing_v), (source, source_v)))
    ]
    for copy in get_small:
        copy.start()

    near = chips // 4
    reach = 4 * near + 2

    barrier = pltpu.get_barrier_semaphore()

    @pl.loop(0, reach - 1)
    def _(j):
        pl.semaphore_signal(
            barrier, inc=1, device_id={"band": peer(reach - 1 - j)}, device_id_type=MESH
        )

    for dx in range(1, n_shell):
        pl.semaphore_signal(
            barrier, inc=1, device_id={"shell": (shell + dx) % n_shell}, device_id_type=MESH
        )

    def get_legendre(i):
        return pltpu.make_async_copy(legendre.at[i], leg_v.at[i], leg_sem.at[i])

    def get_plus(i):
        at = pl.ds(2 * cycles, cycles)
        return pltpu.make_async_copy(plus.at[i], tab_v.at[i, at], plus_sem.at[i])

    def get_minus(i):
        at = pl.ds(3 * cycles, cycles)
        return pltpu.make_async_copy(minus.at[i], tab_v.at[i, at], minus_sem.at[i])

    for i in range(own):
        get_legendre(i).start()
    get_window.start()
    for i in range(own):
        get_plus(i).start()
        get_minus(i).start()

    get_modes.wait()
    for copy in get_small:
        copy.wait()
    for k in range(rows):
        scale = jnp.broadcast_to(weight_v[0:1, k // 2 : k // 2 + 1], (shells, LANES))
        block = modes_v[pl.ds(k, shells, stride=rows), :] * scale
        send_v[pl.ds(k, LANES, stride=rows), :] = block.T

    pl.semaphore_wait(barrier, reach - 1 + n_shell - 1)

    for step in (near, -near):
        pl.semaphore_signal(
            near_sem,
            inc=1,
            device_id={"band": 2 * ((chip + step + chips) % chips) + core},
            device_id_type=MESH,
        )

    def order_copy(i, d):
        return pltpu.make_async_remote_copy(
            src_ref=send_v.at[pl.ds(pl.multiple_of((own * d + i) * rows, rows), rows)],
            dst_ref=recv_v.at[pl.ds(pl.multiple_of((i * n_band + band) * rows, rows), rows)],
            send_sem=send_sem.at[i],
            recv_sem=recv_sem.at[i],
            device_id={"band": d},
            device_id_type=MESH,
        )

    def send(begin, end, orders):
        @pl.loop(0, end - begin)
        def _(k):
            d = peer(end - 1 - k)
            for i in orders:
                order_copy(i, d).start()

    every = range(own)
    early = own // 2
    send(1, reach, range(early))
    pl.semaphore_wait(near_sem, 2)
    for i in every:
        send(reach if i < early else 1, n_band, [i])
    for i in every:
        recv_v[pl.ds(pl.multiple_of((i * n_band + band) * rows, rows), rows), :] = send_v[
            pl.ds(pl.multiple_of((own * band + i) * rows, rows), rows), :
        ]

    def all_orders(i):
        n = (n_band - 1) * rows
        at = pl.ds(pl.multiple_of(i * n_band * rows, rows), n)
        return pltpu.make_async_remote_copy(
            src_ref=recv_v.at[at],
            dst_ref=recv_v.at[at],
            send_sem=send_sem.at[i],
            recv_sem=recv_sem.at[i],
            device_id={"band": 2 * chip + 1 - core},
            device_id_type=MESH,
        )

    spread = jnp.broadcast_to(lensing_v[0:1, :], (LANES, LANES)).T
    shell_id = shell * shells + lax.broadcasted_iota(jnp.int32, (shells, LANES), 0)
    for b in range(bins):
        at = jnp.broadcast_to(source_v[0:1, b : b + 1], (shells, LANES))
        eff_v[b] = spread * jnp.maximum(at - shell_id, 0).astype(f32) / (at + 1).astype(f32)

    sub = lax.broadcasted_iota(jnp.int32, (8, LANES), 0)
    even = sub % 2 == 0

    @pl.loop(0, degrees // LANES)
    def _(k):
        at = pl.multiple_of(k * LANES, LANES)
        degree = (at + lax.broadcasted_iota(jnp.int32, (8, LANES), 1)).astype(f32)
        ratio = jnp.where(
            degree >= 2.0,
            jnp.sqrt((degree + 2.0) * (degree - 1.0) / jnp.maximum(degree * (degree + 1.0), 1.0)),
            0.0,
        )
        fac_v[0:8, pl.ds(at, LANES)] = -ratio
        fac_v[8:16, pl.ds(at, LANES)] = jnp.where(even, ratio, -ratio)

    @pl.loop(0, own)
    def _(i):
        get_legendre(i).wait()

        @pl.loop(0, cycles // 16)
        def _(k):
            at = pl.ds(pl.multiple_of(k * 16, 16), 16)
            value = leg_v[i, at, :]
            high = value.astype(bf16)
            tab_v[i, at, :] = high
            at = pl.ds(pl.multiple_of(cycles + k * 16, 16), 16)
            tab_v[i, at, :] = (value - high.astype(f32)).astype(bf16)

    get_window.wait()

    def transform(i, t, h_v):
        table = tab_v[i, 0 : 2 * cycles, pl.ds(pl.multiple_of(t * TILE, TILE), TILE)]
        h_v[...] = jnp.dot(a_v[...], table, preferred_element_type=f32) + jnp.dot(
            x_v[...], table[:cycles], preferred_element_type=f32
        )

    def merge(x, y, s):
        clear = (sub & s) == 0
        if s == 4:
            return jnp.where(clear, x, y) + roll(jnp.where(clear, y, x), 4, 0)
        return jnp.where(clear, x, y) + jnp.where(clear, roll(x, 8 - s, 0), roll(y, s, 0))

    def bin_sums(t, h_v):
        for k in range(TILE // LANES):
            lanes = pl.ds(pl.multiple_of(t * TILE + k * LANES, LANES), LANES)
            sums = [[None, None] for _ in range(bins)]
            for g in range(shells // 8):
                at = slice(8 * g, 8 * g + 8)
                w = win_v[at, lanes]
                for c in range(2):
                    h = h_v[c * shells + 8 * g : c * shells + 8 * g + 8, k * LANES : (k + 1) * LANES]
                    hw = h * w
                    for b in range(bins):
                        term = hw * eff_v[b, at, :]
                        sums[b][c] = term if g == 0 else sums[b][c] + term
            z = [[merge(sums[b][c], sums[b + 2][c], 4) for c in range(2)] for b in range(2)]
            z = [merge(z[0][c], z[1][c], 2) for c in range(2)]
            z = merge(z[0], z[1], 1)
            low = z - z.astype(bf16).astype(f32)
            turned = jnp.where(even, roll(z, 7, 0), roll(z, 1, 0))
            w_v[:, lanes] = jnp.concatenate(
                [z, low, z * fac_v[0:8, lanes], turned * fac_v[8:16, lanes]], axis=0
            ).astype(bf16)

    def products(i, t):
        at = pl.ds(pl.multiple_of(t * 2 * TILE, 2 * TILE), 2 * TILE)
        return lax.dot_general(
            tab_v[i, :, at], w_v[:, at], (((1,), (1,)), ((), ())), preferred_element_type=f32
        )

    pairs = degrees // (2 * TILE)

    def pair(i, t):
        transform(i, 2 * t + 1, h1_v)
        bin_sums(2 * t, h0_v)
        if not isinstance(t, int) or t < pairs - 1:
            transform(i, 2 * t + 2, h0_v)
        bin_sums(2 * t + 1, h1_v)

    @pl.loop(0, own)
    def _(i):
        all_orders(i).wait_recv()
        for c in range(2):
            x = recv_v[pl.ds(i * n_band * rows + c, cycles, stride=2), :].T
            high = x.astype(bf16)
            at = slice(c * shells, (c + 1) * shells)
            a_v[at, :cycles] = high
            a_v[at, cycles:] = high
            x_v[at, :] = (x - high.astype(f32)).astype(bf16)

        get_plus(i).wait()
        get_minus(i).wait()
        transform(i, 0, h0_v)
        pair(i, 0)
        m_v[...] = jnp.zeros_like(m_v)

        @pl.loop(1, pairs - 1)
        def _(t):
            m_v[...] += products(i, t - 1)
            pair(i, t)

        m_v[...] += products(i, pairs - 2)
        pair(i, pairs - 1)
        maps = (m_v[...] + products(i, pairs - 1)).T
        field = [maps[:, q * cycles : (q + 1) * cycles] for q in range(4)]
        kappa = field[0][0:8] + field[0][8:16] + field[1][0:8]
        p, m = field[2][16:24], field[3][24:32]
        for b in range(bins):
            k0, p0, m0 = (
                x if n % 8 == 0 else roll(x, n % 8, 0)
                for x, n in ((kappa, 8 - 2 * b), (p, 10 - 2 * b), (m, 12 - 2 * b))
            )
            p1s_v[i, b] = jnp.where(sub < 2, k0, jnp.where(sub < 4, p0, m0))
        for dx in sorted(range(1, n_shell), key=lambda x: abs(2 * x - n_shell)):
            d = lax.rem(shell + dx, n_shell)
            pltpu.make_async_remote_copy(
                src_ref=p1s_v.at[i, d],
                dst_ref=p1r_v.at[i, shell],
                send_sem=p1s_sem.at[i],
                recv_sem=p1r_sem.at[i],
                device_id={"shell": d},
                device_id_type=MESH,
            ).start()
        p1r_v[i, shell] = p1s_v[i, shell]

    def all_bins(i):
        return pltpu.make_async_remote_copy(
            src_ref=p1r_v.at[i, pl.ds(0, n_shell - 1)],
            dst_ref=p1r_v.at[i, pl.ds(0, n_shell - 1)],
            send_sem=p1s_sem.at[i],
            recv_sem=p1r_sem.at[i],
            device_id={"shell": (shell + 1) % n_shell},
            device_id_type=MESH,
        )

    summed = []
    for i in range(own):
        all_bins(i).wait_recv()
        total = p1r_v[i, 0]
        for x in range(1, n_shell):
            total = total + p1r_v[i, x]
        summed.append(total)
    width = 8 * own
    summed.append(jnp.zeros((LANES - width, LANES), f32))
    p2t_v[...] = jnp.concatenate(summed, axis=0).T
    per = cycles // n_band
    packed = p2t_v[pl.ds(0, n_band, stride=per), :]
    for q in range(1, per):
        packed = packed + roll(p2t_v[pl.ds(q, n_band, stride=per), :], q * width, 1)
    for d in range(n_band):
        p2s_v[d] = packed[d : d + 1]

    @pl.loop(1, n_band)
    def _(j):
        d = peer(n_band - j)
        pltpu.make_async_remote_copy(
            src_ref=p2s_v.at[d],
            dst_ref=p2r_v.at[band],
            send_sem=p2s_sem,
            recv_sem=p2r_sem,
            device_id={"band": d},
            device_id_type=MESH,
        ).start()

    p2r_v[band] = p2s_v[band]
    last = pltpu.make_async_remote_copy(
        src_ref=p2r_v.at[pl.ds(0, n_band - 1)],
        dst_ref=p2r_v.at[pl.ds(0, n_band - 1)],
        send_sem=p2s_sem,
        recv_sem=p2r_sem,
        device_id={"band": 2 * chip + 1 - core},
        device_id_type=MESH,
    )
    last.wait_recv()
    got = jnp.concatenate(
        [p2r_v[d] for d in range(n_band)] + [jnp.zeros((LANES - n_band, LANES), f32)], axis=0
    ).T
    lane = lax.broadcasted_iota(jnp.int32, (8, LANES), 1)
    for q in range(per):
        field = jnp.zeros((8, LANES), f32)
        for i in range(own):
            block = got[(q * own + i) * 8 : (q * own + i) * 8 + 8]
            block = jnp.take_along_axis(block, lane // own, axis=1)
            field = jnp.where(lane % own == i, block, field)
        for f in range(3):
            at = f * 2 * per + 2 * q
            out[at : at + 2, :] = field[2 * f : 2 * f + 2]
    for i in range(own):
        all_orders(i).wait_send()
        all_bins(i).wait_send()
    last.wait_send()


def on_device(n_band, n_shell, modes, weight, legendre, plus, minus, window, lensing, source):
    f32, bf16 = jnp.float32, jnp.bfloat16
    own, cycles, degrees = legendre.shape
    shells, per, parts, orders = modes.shape
    rows = per * parts
    bins = n_shell
    vmem, hbm = pltpu.VMEM, pl.ANY
    dma = pltpu.SemaphoreType.DMA
    maps = pl.pallas_call(
        functools.partial(kernel, n_band, n_shell),
        out_shape=vmem((3 * rows, orders), f32),
        in_specs=[pl.BlockSpec(memory_space=hbm)] * 8,
        out_specs=pl.BlockSpec(memory_space=vmem),
        scratch_shapes=[
            vmem((1, per), f32),
            vmem((1, shells), f32),
            vmem((1, bins), jnp.int32),
            vmem((shells * rows, orders), f32),
            vmem((orders * rows, shells), f32),
            vmem((orders * rows, shells), f32),
            vmem((own, cycles, degrees), f32),
            vmem((own, 4 * cycles, degrees), bf16),
            vmem((shells, degrees), f32),
            vmem((bins, shells, LANES), f32),
            vmem((16, degrees), f32),
            vmem((2 * shells, 2 * cycles), bf16),
            vmem((2 * shells, cycles), bf16),
            vmem((2 * shells, TILE), f32),
            vmem((2 * shells, TILE), f32),
            vmem((8 * bins, degrees), bf16),
            vmem((4 * cycles, 8 * bins), f32),
            vmem((own, n_shell, 8, LANES), f32),
            vmem((own, n_shell, 8, LANES), f32),
            vmem((cycles, LANES), f32),
            vmem((n_band, 1, LANES), f32),
            vmem((n_band, 1, LANES), f32),
            pltpu.SemaphoreType.REGULAR,
            dma((5,)),
            dma((own,)),
            dma((own,)),
            dma((own,)),
            dma((own,)),
            dma((own,)),
            dma((own,)),
            dma((own,)),
            dma,
            dma,
        ],
        compiler_params=pltpu.CompilerParams(
            collective_id=0, has_side_effects=True, vmem_limit_bytes=60 * 2**20
        ),
    )(
        modes.reshape(shells * rows, orders),
        weight.reshape(1, per),
        legendre,
        plus,
        minus,
        window,
        lensing.reshape(1, shells),
        source.reshape(1, bins),
    )
    return maps.reshape(1, 3, per, parts, orders)


def solution(mesh):
    in_specs = (
        P(("cosmo", "shell"), "band", None, None),
        P("band"),
        P("band", None, None),
        P("band", None, None),
        P("band", None, None),
        P("shell", None),
        P(("cosmo", "shell")),
        P("cosmo"),
    )
    out_specs = P(("cosmo", "shell"), None, "band", None, None)
    return jax.shard_map(
        functools.partial(on_device, mesh.shape["band"], mesh.shape["shell"]),
        mesh=mesh,
        in_specs=in_specs,
        out_specs=out_specs,
        check_vma=False,
    )
```
